32 devices in a mesh: seq: 8 (over z, x), head: 4 (over y, core).
Axes of the slice: x: 2, y: 2, z: 4, core: 2. Of those that a mesh axis runs over, the one named last changes fastest.
Arguments:
- tokens: bfloat16 [8192, 2048], P('seq', 'head'), may hold values from -8 to 8
- w_query: bfloat16 [2048, 2048], P(None, 'head'), may hold values from -1 to 1, as said below
- w_key: bfloat16 [2048, 2048], P(None, 'head'), may hold values from -1 to 1, as said below
- w_value: bfloat16 [2048, 2048], P(None, 'head'), may hold values from -0.125 to 0.125
- w_out: bfloat16 [2048, 2048], P('head'), may hold values from -0.125 to 0.125
- mix_logit: float32 [8], P('head'), may hold values from -2 to 2
Outputs:
- layer_out: bfloat16 [8192, 2048], P('seq', 'head')
The draws below stay inside these ranges and needn't reach their ends.
Inputs may be any that keep to these rules, and one draw needn't show every extreme that they name: `w_query`: entries of mean zero with a standard deviation of about 2048 ** -0.5. `w_key`: entries of mean zero with a standard deviation of about 2048 ** -0.5.
All inputs are finite; a program needn't handle non-finite values.
Results may differ from the reference program's by a relative error of at most 0.0065.
Values may be sent and summed in bfloat16 or wider, within the bound.
A program may use at most 128 MiB of HBM per device.

```python
import jax
import jax.numpy as jnp
from jax import lax

D = 2048
H = 8
DH = 256
SEG_DEV = 1024
TOKENS = 8192


def query_key_pair(key):
    scale = D ** (-0.5)
    base = jnp.clip(jax.random.normal(jax.random.fold_in(key, 31), (D, H * DH), jnp.float32), -4.5, 4.5)
    other = jnp.clip(jax.random.normal(jax.random.fold_in(key, 32), (D, H * DH), jnp.float32), -4.5, 4.5)
    second = other
    return ((base * scale).astype(jnp.bfloat16), (second * scale).astype(jnp.bfloat16))


def draw_w_query(key, part):
    return query_key_pair(key)[0]


def draw_w_key(key, part):
    return query_key_pair(key)[1]


def draw_tokens(key, part):
    nseg = TOKENS // SEG_DEV
    offsets = jax.random.normal(jax.random.fold_in(key, 11), (nseg, 1, D), jnp.float32)
    base = jax.random.normal(jax.random.fold_in(key, 14), (nseg, SEG_DEV, D), jnp.float32)
    whole = base + 0.7 * offsets
    return jnp.clip(whole, -8.0, 8.0).reshape(TOKENS, D).astype(jnp.bfloat16)


def steps_of(stream_key, shape, cuts, smallest, largest):
    loudness, own = 1.0, jax.random.fold_in(stream_key, 6)
    for dim, shards_of in cuts:
        draws = jnp.exp(jax.random.uniform(jax.random.fold_in(own, dim), (shards_of,), jnp.float32, smallest / len(cuts), largest / len(cuts)))
        loudness = loudness * jnp.repeat(draws, shape[dim] // shards_of).reshape([-1 if axis == dim else 1 for axis in range(len(shape))])
    return loudness


def bell_draw(stream_key, shape, scale, limit, split=(), kind=jnp.bfloat16):
    values = scale * jax.random.normal(stream_key, shape, jnp.float32)
    if split:
        values = values * steps_of(stream_key, shape, split, -0.22, 0.18)
    return jnp.clip(values, -limit, limit).astype(kind)


def setup_inputs(seed: int = 0) -> dict:
    key_of = jax.random.split(jax.random.key(seed), 7)
    return {
        "tokens": draw_tokens(jax.random.fold_in(key_of[6], 71), 0),
        "w_query": draw_w_query(jax.random.fold_in(key_of[6], 71), 0),
        "w_key": draw_w_key(jax.random.fold_in(key_of[6], 71), 0),
        "w_value": bell_draw(key_of[3], (D, H * DH), D ** -0.5, 0.125, ((1, 4),)),
        "w_out": bell_draw(key_of[4], (H * DH, D), (H * DH) ** -0.5, 0.125, ((0, 4),)),
        "mix_logit": jnp.clip(jax.random.uniform(key_of[5], (H,), jnp.float32, -2.0, 2.0) * steps_of(key_of[5], (H,), ((0, 4),), -0.4, 0.0), -2.0, 2.0),
    }


def feature(values):
    return jax.nn.elu(values) + 1.0


def reference(tokens, w_query, w_key, w_value, w_out, mix_logit):
    nseg = TOKENS // SEG_DEV
    blocks = tokens.reshape(nseg, SEG_DEV, D)
    share = jax.nn.sigmoid(mix_logit)[None, :, None]
    rows = lax.broadcasted_iota(jnp.int32, (SEG_DEV, SEG_DEV), 0)
    cols = lax.broadcasted_iota(jnp.int32, (SEG_DEV, SEG_DEV), 1)
    causal = cols <= rows
    scale = 1.0 / (DH ** 0.5)

    def one(carry, block):
        memory, normal = carry
        query = jnp.dot(block, w_query, preferred_element_type=jnp.float32).astype(jnp.bfloat16).reshape(SEG_DEV, H, DH)
        keys = jnp.dot(block, w_key, preferred_element_type=jnp.float32).astype(jnp.bfloat16).reshape(SEG_DEV, H, DH)
        values = jnp.dot(block, w_value, preferred_element_type=jnp.float32).astype(jnp.bfloat16).reshape(SEG_DEV, H, DH)
        scores = jnp.einsum("qhd,khd->hqk", query.astype(jnp.float32), keys.astype(jnp.float32)) * scale
        scores = jnp.where(causal[None], scores, -1e30)
        expo = jnp.exp(scores - jnp.max(scores, axis=2, keepdims=True))
        probs = (expo / jnp.sum(expo, axis=2, keepdims=True)).astype(jnp.bfloat16)
        local = jnp.einsum("hqk,khd->qhd", probs.astype(jnp.float32), values.astype(jnp.float32))
        fquery = feature(query.astype(jnp.float32)).astype(jnp.bfloat16).astype(jnp.float32)
        fkey = feature(keys.astype(jnp.float32)).astype(jnp.bfloat16).astype(jnp.float32)
        numer = jnp.einsum("thd,hde->the", fquery, memory, precision=lax.Precision.HIGHEST)
        denom = jnp.einsum("thd,hd->th", fquery, normal, precision=lax.Precision.HIGHEST)
        readout = numer / jnp.maximum(denom, 1.0)[:, :, None]
        mixed = (share * readout + (1.0 - share) * local).astype(jnp.bfloat16).reshape(SEG_DEV, H * DH)
        result = jnp.dot(mixed, w_out, preferred_element_type=jnp.float32).astype(jnp.bfloat16)
        memory = memory + jnp.einsum("thd,the->hde", fkey, values.astype(jnp.float32))
        normal = normal + jnp.sum(fkey, axis=0)
        return (memory, normal), result

    start = (jnp.zeros((H, DH, DH), jnp.float32), jnp.zeros((H, DH), jnp.float32))
    carry, outs = lax.scan(one, start, blocks)
    return outs.reshape(TOKENS, D)
```

```python
import functools

import jax
import jax.numpy as jnp
from jax import lax
from jax.experimental import pallas as pl
from jax.experimental.pallas import tpu as pltpu
from jax.sharding import PartitionSpec as P

MESH = pl.DeviceIdType.MESH
CHUNKS = 4
PAD = 16
BF16 = jnp.bfloat16
F32 = jnp.float32


def feature(values):
    return jnp.where(values > 0.0, values + 1.0, jnp.exp(jnp.minimum(values, 0.0)))


def matmul(a, b):
    return jnp.dot(a, b, preferred_element_type=F32)


def kernel(
    groups, tok, wq, wk, wv, wo, logit, out,
    x, w, wos, q, k, v, loc, mix, psend, precv, outv, term, s1send, s1recv, s2send, s2recv, s3send, memory,
    tok_sem, w_sem, wo_sem, wos_s, wos_r, sib_s, sib_r, cross_s, cross_r, far_s, far_r,
    e1_s, e1_r, e2_s, e2_r, e3_s, e3_r, mix_s, mix_r, p_s, p_r, out_sem,
):
    seg, feats = tok.shape
    width = wq.shape[1]
    heads = logit.shape[0]
    hsize = width // heads
    half = heads // 2
    rows_of = seg // CHUNKS
    here, sq = lax.axis_index("head"), lax.axis_index("seq")
    sib = here + 1 - 2 * lax.rem(here, 2)
    cross = lax.rem(here + 2, 4)
    far = lax.rem(sib + 2, 4)
    b, a = lax.rem(sq, 2), lax.div(sq, 2)
    pair = sq + 1 - 2 * b

    def rows(i):
        return pl.ds(i * rows_of, rows_of)

    def block(index, size):
        return pl.ds(pl.multiple_of(index * size, size), size)

    def remote(src, dst, send, recv, head=None, seq=None):
        target = (sq if seq is None else seq, here if head is None else head)
        return pltpu.make_async_remote_copy(
            src_ref=src, dst_ref=dst, send_sem=send, recv_sem=recv, device_id=target, device_id_type=MESH
        )

    own_tok = [
        pltpu.make_async_copy(tok.at[rows(i), :], x.at[rows(i), pl.ds(0, feats)], tok_sem.at[i]) for i in range(CHUNKS)
    ]
    own_tok[0].start()
    order = (here, sib, cross, far)
    weights = []
    for slot, device in enumerate(order):
        for t, weight in enumerate((wq, wk, wv)):
            copy = pltpu.make_async_copy(
                weight.at[block(device, feats), :], w.at[t, pl.ds(slot * feats, feats), :], w_sem.at[t, slot]
            )
            copy.start()
            weights.append(copy)
    for copy in own_tok[1:]:
        copy.start()
    own_wo = [
        pltpu.make_async_copy(
            wo.at[:, block(device, feats)], wos.at[pl.ds(0, width), pl.ds(j * feats, feats)], wo_sem.at[j]
        )
        for j, device in enumerate((here, cross))
    ]
    for copy in own_wo:
        copy.start()

    barrier = pltpu.get_barrier_semaphore()
    partners = [(sq, sib), (sq, cross), (pair, here)]
    for d in range(1, groups):
        partners.append((2 * lax.rem(a + d, groups) + b, here))
    for partner in partners:
        pl.semaphore_signal(barrier, inc=1, device_id=partner, device_id_type=MESH)
    pl.semaphore_wait(barrier, len(partners))

    to_cross = [
        remote(tok.at[rows(i), :], x.at[rows(i), pl.ds(2 * feats, feats)], cross_s.at[i], cross_r.at[i], head=cross)
        for i in range(CHUNKS)
    ]
    to_sib = [
        remote(tok.at[rows(i), :], x.at[rows(i), pl.ds(feats, feats)], sib_s.at[i], sib_r.at[i], head=sib)
        for i in range(CHUNKS)
    ]
    forward = [
        remote(
            x.at[rows(i), pl.ds(2 * feats, feats)],
            x.at[rows(i), pl.ds(3 * feats, feats)],
            far_s.at[i],
            far_r.at[i],
            head=sib,
        )
        for i in range(CHUNKS)
    ]
    for i in range(CHUNKS):
        to_cross[i].start()
        to_sib[i].start()
    to_wos = [
        remote(
            wo.at[:, block(device, feats)],
            wos.at[pl.ds(width, width), pl.ds(j * feats, feats)],
            wos_s.at[j],
            wos_r.at[j],
            head=sib,
        )
        for j, device in enumerate((sib, far))
    ]
    for copy in to_wos:
        copy.start()

    term[...] = jnp.zeros_like(term)
    scale = 1.0 / hsize**0.5

    def attention(i, h):
        cols = pl.ds(h * hsize, hsize)
        query = q[rows(i), cols]
        spot = lax.broadcasted_iota(jnp.int32, (rows_of, rows_of), 0)
        causal = lax.broadcasted_iota(jnp.int32, (rows_of, rows_of), 1) <= spot

        def scores_of(span):
            return lax.dot_general(query, k[span, cols], (((1,), (1,)), ((), ())), preferred_element_type=F32) * scale

        last = jnp.where(causal, scores_of(rows(i)), -1e30)
        top = jnp.max(last, axis=1, keepdims=True)
        if i:
            before = pl.ds(0, i * rows_of)
            first = scores_of(before)
            top = jnp.maximum(top, jnp.max(first, axis=1, keepdims=True))
        expo = jnp.exp(last - top)
        total = jnp.sum(expo, axis=1, keepdims=True)
        value = matmul(expo.astype(BF16), v[rows(i), cols])
        if i:
            expo = jnp.exp(first - top)
            total = total + jnp.sum(expo, axis=1, keepdims=True)
            value = value + matmul(expo.astype(BF16), v[before, cols])
        loc[rows(i), cols] = value / total

    for i in range(CHUNKS):
        to_cross[i].wait_recv()
        forward[i].start()
        if i:
            for h in range(heads):
                attention(i - 1, h)
        own_tok[i].wait()
        to_sib[i].wait_recv()
        if i == 0:
            for copy in weights:
                copy.wait()
        forward[i].wait_recv()
        for t, target in ((1, k), (2, v)):
            target[rows(i), :] = matmul(x[rows(i), :], w[t]).astype(BF16)
        for h in range(heads):
            cols = pl.ds(h * hsize, hsize)
            fkey = feature(k[rows(i), cols].astype(F32)).astype(BF16)
            term[h, pl.ds(0, hsize), :] += lax.dot_general(
                fkey, v[rows(i), cols], (((0,), (0,)), ((), ())), preferred_element_type=F32
            )
            term[h, pl.ds(hsize, PAD), :] += jnp.broadcast_to(
                jnp.sum(fkey.astype(F32), axis=0, keepdims=True), (PAD, hsize)
            )
        if i < CHUNKS - 1:
            q[rows(i), :] = matmul(x[rows(i), :], w[0]).astype(BF16)

    mine, other = pl.ds(b * half, half), pl.ds((1 - b) * half, half)
    s1send[...] = term[other].astype(BF16)
    swap = remote(s1send, s1recv, e1_s, e1_r, seq=pair)
    swap.start()
    q[rows(CHUNKS - 1), :] = matmul(x[rows(CHUNKS - 1), :], w[0]).astype(BF16)
    swap.wait_recv()
    s2send[...] = (term[mine] + s1recv[...].astype(F32)).astype(BF16)

    def later(d):
        return remote(s2send, s2recv.at[a], e2_s.at[d], e2_r.at[a], seq=sq + 2 * d)

    for d in range(1, groups):

        @pl.when(a + d < groups)
        def _(d=d):
            later(d).start()

    for h in range(heads):
        attention(CHUNKS - 1, h)

    s3 = jnp.where(b == 0, term[mine], 0.0)
    term[other] = jnp.where(b == 1, s1recv[...].astype(F32), 0.0)
    term[mine] = s3
    for g in range(groups - 1):

        @pl.when(g < a)
        def _(g=g):
            remote(s2send, s2recv.at[g], e2_s.at[0], e2_r.at[g], seq=pair).wait_recv()
            got = s2recv[g].astype(F32)
            term[mine] += got
            term[other] += got

    s3send[...] = term[mine].astype(BF16)
    back = remote(s3send, memory.at[mine], e3_s, e3_r, seq=pair)
    back.start()
    memory[mine] = term[other].astype(BF16)

    to_mix = [
        remote(
            mix.at[rows(i), pl.ds(0, width)], mix.at[rows(i), pl.ds(width, width)], mix_s.at[i], mix_r.at[i], head=sib
        )
        for i in range(CHUNKS)
    ]
    to_p = [remote(psend.at[rows(i), :], precv.at[rows(i), :], p_s.at[i], p_r.at[i], head=cross) for i in range(CHUNKS)]
    to_out = [pltpu.make_async_copy(outv.at[rows(i), :], out.at[rows(i), :], out_sem.at[i]) for i in range(CHUNKS)]

    def readout(i):
        for h in range(heads):
            cols = pl.ds(h * hsize, hsize)
            share = jax.nn.sigmoid(jnp.full((1, hsize), logit[h], F32))
            fquery = feature(q[rows(i), cols].astype(F32)).astype(BF16)
            numer = matmul(fquery, memory[h, pl.ds(0, hsize), :])
            normal = memory[h, pl.ds(hsize, PAD), :].astype(F32)[0:1]
            denom = jnp.sum(fquery.astype(F32) * normal, axis=1, keepdims=True)
            read = numer / jnp.maximum(denom, 1.0)
            mix[rows(i), cols] = (share * read + (1.0 - share) * loc[rows(i), cols]).astype(BF16)
        to_mix[i].start()

    def partial(i):
        to_mix[i].wait_recv()
        if i == 0:
            for copy in own_wo:
                copy.wait()
            for copy in to_wos:
                copy.wait_recv()
        psend[rows(i), :] = matmul(mix[rows(i), :], wos[:, pl.ds(feats, feats)]).astype(BF16)
        to_p[i].start()

    back.wait_recv()
    readout(0)
    for i in range(1, CHUNKS):
        readout(i)
        partial(i - 1)
    partial(CHUNKS - 1)
    for i in range(CHUNKS):
        own = matmul(mix[rows(i), :], wos[:, pl.ds(0, feats)])
        to_p[i].wait_recv()
        outv[rows(i), :] = (own + precv[rows(i), :].astype(F32)).astype(BF16)
        to_out[i].start()

    for i in range(CHUNKS):
        for copies in (to_cross, to_sib, forward, to_mix, to_p):
            copies[i].wait_send()
    for copy in to_wos + [swap, back]:
        copy.wait_send()
    for d in range(1, groups):

        @pl.when(a + d < groups)
        def _(d=d):
            later(d).wait_send()

    for copy in to_out:
        copy.wait()


def on_device(groups, tokens, w_query, w_key, w_value, w_out, mix_logit):
    seg, feats = tokens.shape
    depth, width = w_query.shape
    heads = mix_logit.shape[0]
    hsize = width // heads
    half = heads // 2
    dma = pltpu.SemaphoreType.DMA
    piece = (half, hsize + PAD, hsize)
    anywhere = pl.BlockSpec(memory_space=pl.ANY)
    return pl.pallas_call(
        functools.partial(kernel, groups),
        out_shape=jax.ShapeDtypeStruct((seg, feats), BF16),
        in_specs=[anywhere] * 5 + [pl.BlockSpec(memory_space=pltpu.SMEM)],
        out_specs=anywhere,
        scratch_shapes=[
            pltpu.VMEM((seg, depth), BF16),
            pltpu.VMEM((3, depth, width), BF16),
            pltpu.VMEM((2 * width, 2 * feats), BF16),
            pltpu.VMEM((seg, width), BF16),
            pltpu.VMEM((seg, width), BF16),
            pltpu.VMEM((seg, width), BF16),
            pltpu.VMEM((seg, width), F32),
            pltpu.VMEM((seg, 2 * width), BF16),
            pltpu.VMEM((seg, feats), BF16),
            pltpu.VMEM((seg, feats), BF16),
            pltpu.VMEM((seg, feats), BF16),
            pltpu.VMEM((heads, hsize + PAD, hsize), F32),
            pltpu.VMEM(piece, BF16),
            pltpu.VMEM(piece, BF16),
            pltpu.VMEM(piece, BF16),
            pltpu.VMEM((groups,) + piece, BF16),
            pltpu.VMEM(piece, BF16),
            pltpu.VMEM((heads, hsize + PAD, hsize), BF16),
            dma((CHUNKS,)),
            dma((3, 4)),
            dma((2,)),
            dma((2,)),
            dma((2,)),
        ]
        + [dma((CHUNKS,))] * 6
        + [dma, dma, dma((groups,)), dma((groups,)), dma, dma]
        + [dma((CHUNKS,))] * 5,
        compiler_params=pltpu.CompilerParams(collective_id=0, has_side_effects=True, vmem_limit_bytes=64000000),
    )(tokens, w_query, w_key, w_value, w_out, mix_logit)


def solution(mesh):
    placed = (
        P("seq", "head"),
        P(None, "head"),
        P(None, "head"),
        P(None, "head"),
        P("head", None),
        P("head"),
    )
    return jax.shard_map(
        functools.partial(on_device, mesh.shape["seq"] // 2),
        mesh=mesh,
        in_specs=placed,
        out_specs=P("seq", "head"),
        check_vma=False,
    )
```

```python
import functools

import jax
import jax.numpy as jnp
from jax import lax
from jax.experimental import pallas as pl
from jax.experimental.pallas import tpu as pltpu
from jax.sharding import PartitionSpec as P

MESH = pl.DeviceIdType.MESH
CHUNKS = 8
PIECES = 8
PAD = 16
BF16 = jnp.bfloat16
F32 = jnp.float32


def feature(values):
    return jnp.where(values > 0.0, values + 1.0, jnp.exp(jnp.minimum(values, 0.0)))


def matmul(a, b):
    return jnp.dot(a, b, preferred_element_type=F32)


def kernel(
    groups, tok, wq, wk, wv, wo, logit, out,
    x, w, wos, q, k, v, loc, mix, psend, precv, outv, term, s1send, s1recv, s2send, s2recv, s3send, memory,
    tok_sem, w_sem, wo_sem, wos_s, wos_r, sib_s, sib_r, cross_s, cross_r, far_s, far_r,
    e1_s, e1_r, e2_s, e2_r, e3_s, e3_r, mix_s, mix_r, p_s, p_r, out_sem,
):
    seg, feats = tok.shape
    width = wq.shape[1]
    heads = logit.shape[0]
    hsize = width // heads
    half = heads // 2
    rows_of = seg // CHUNKS
    here, sq = lax.axis_index("head"), lax.axis_index("seq")
    sib = here + 1 - 2 * lax.rem(here, 2)
    cross = lax.rem(here + 2, 4)
    far = lax.rem(sib + 2, 4)
    b, a = lax.rem(sq, 2), lax.div(sq, 2)
    pair = sq + 1 - 2 * b

    def rows(i):
        return pl.ds(i * rows_of, rows_of)

    def block(index, size):
        return pl.ds(pl.multiple_of(index * size, size), size)

    def remote(src, dst, send, recv, head=None, seq=None):
        target = (sq if seq is None else seq, here if head is None else head)
        return pltpu.make_async_remote_copy(
            src_ref=src, dst_ref=dst, send_sem=send, recv_sem=recv, device_id=target, device_id_type=MESH
        )

    own_tok = [
        pltpu.make_async_copy(tok.at[rows(i), :], x.at[rows(i), pl.ds(0, feats)], tok_sem.at[i]) for i in range(CHUNKS)
    ]
    own_tok[0].start()
    order = (here, sib, cross, far)
    weights = []
    for slot, device in enumerate(order):
        for t, weight in enumerate((wq, wk, wv)):
            copy = pltpu.make_async_copy(
                weight.at[block(device, feats), :], w.at[t, pl.ds(slot * feats, feats), :], w_sem.at[t, slot]
            )
            copy.start()
            weights.append(copy)
    for copy in own_tok[1:]:
        copy.start()
    own_wo = [
        pltpu.make_async_copy(
            wo.at[:, block(device, feats)], wos.at[pl.ds(0, width), pl.ds(j * feats, feats)], wo_sem.at[j]
        )
        for j, device in enumerate((here, cross))
    ]
    for copy in own_wo:
        copy.start()

    barrier = pltpu.get_barrier_semaphore()
    partners = [(sq, sib), (sq, cross), (pair, here)]
    for d in (1, groups - 1):
        partners.append((2 * lax.rem(a + d, groups) + b, here))
    for partner in partners:
        pl.semaphore_signal(barrier, inc=1, device_id=partner, device_id_type=MESH)
    pl.semaphore_wait(barrier, len(partners))

    to_cross = [
        remote(tok.at[rows(i), :], x.at[rows(i), pl.ds(2 * feats, feats)], cross_s.at[i], cross_r.at[i], head=cross)
        for i in range(CHUNKS)
    ]
    to_sib = [
        remote(tok.at[rows(i), :], x.at[rows(i), pl.ds(feats, feats)], sib_s.at[i], sib_r.at[i], head=sib)
        for i in range(CHUNKS)
    ]
    forward = [
        remote(
            x.at[rows(i), pl.ds(2 * feats, feats)],
            x.at[rows(i), pl.ds(3 * feats, feats)],
            far_s.at[i],
            far_r.at[i],
            head=sib,
        )
        for i in range(CHUNKS)
    ]
    for i in range(CHUNKS):
        to_cross[i].start()
        to_sib[i].start()
    to_wos = [
        remote(
            wo.at[:, block(device, feats)],
            wos.at[pl.ds(width, width), pl.ds(j * feats, feats)],
            wos_s.at[j],
            wos_r.at[j],
            head=sib,
        )
        for j, device in enumerate((sib, far))
    ]
    for copy in to_wos:
        copy.start()

    term[...] = jnp.zeros_like(term)
    scale = 1.0 / hsize**0.5

    def attention(i, h):
        cols = pl.ds(h * hsize, hsize)
        query = q[rows(i), cols]
        spot = lax.broadcasted_iota(jnp.int32, (rows_of, rows_of), 0)
        causal = lax.broadcasted_iota(jnp.int32, (rows_of, rows_of), 1) <= spot

        def scores_of(span):
            return lax.dot_general(query, k[span, cols], (((1,), (1,)), ((), ())), preferred_element_type=F32) * scale

        last = jnp.where(causal, scores_of(rows(i)), -1e30)
        top = jnp.max(last, axis=1, keepdims=True)
        if i:
            before = pl.ds(0, i * rows_of)
            first = scores_of(before)
            top = jnp.maximum(top, jnp.max(first, axis=1, keepdims=True))
        expo = jnp.exp(last - top)
        total = jnp.sum(expo, axis=1, keepdims=True)
        value = matmul(expo.astype(BF16), v[rows(i), cols])
        if i:
            expo = jnp.exp(first - top)
            total = total + jnp.sum(expo, axis=1, keepdims=True)
            value = value + matmul(expo.astype(BF16), v[before, cols])
        loc[rows(i), cols] = value / total

    for i in range(CHUNKS):
        to_cross[i].wait_recv()
        forward[i].start()
        if i:
            for h in range(heads):
                attention(i - 1, h)
        own_tok[i].wait()
        to_sib[i].wait_recv()
        if i == 0:
            for copy in weights:
                copy.wait()
        forward[i].wait_recv()
        for t, target in ((1, k), (2, v)):
            target[rows(i), :] = matmul(x[rows(i), :], w[t]).astype(BF16)
        for h in range(heads):
            cols = pl.ds(h * hsize, hsize)
            fkey = feature(k[rows(i), cols].astype(F32)).astype(BF16)
            term[h, pl.ds(0, hsize), :] += lax.dot_general(
                fkey, v[rows(i), cols], (((0,), (0,)), ((), ())), preferred_element_type=F32
            )
            term[h, pl.ds(hsize, PAD), :] += jnp.broadcast_to(
                jnp.sum(fkey.astype(F32), axis=0, keepdims=True), (PAD, hsize)
            )
        if i < CHUNKS - 1:
            q[rows(i), :] = matmul(x[rows(i), :], w[0]).astype(BF16)

    mine, other = pl.ds(b * half, half), pl.ds((1 - b) * half, half)
    step = hsize // PIECES
    spans = [pl.ds(p * step, step + (PAD if p == PIECES - 1 else 0)) for p in range(PIECES)]
    swap = [
        remote(s1send.at[:, span], s1recv.at[:, span], e1_s.at[p], e1_r.at[p], seq=pair)
        for p, span in enumerate(spans)
    ]
    chain = [
        remote(s2send.at[:, span], s2recv.at[:, span], e2_s.at[p], e2_r.at[p], seq=sq + 2)
        for p, span in enumerate(spans)
    ]
    back = [
        remote(s3send.at[:, span], memory.at[mine, span], e3_s.at[p], e3_r.at[p], seq=pair)
        for p, span in enumerate(spans)
    ]
    for p, span in enumerate(spans):
        s1send[:, span] = term[other, span].astype(BF16)
        swap[p].start()

    @pl.when(a == 0)
    def _():
        s2recv[...] = jnp.zeros_like(s2recv)

    q[rows(CHUNKS - 1), :] = matmul(x[rows(CHUNKS - 1), :], w[0]).astype(BF16)
    for p, span in enumerate(spans):
        swap[p].wait_recv()

        @pl.when(a > 0)
        def _(p=p):
            chain[p].wait_recv()

        own = term[mine, span]
        paired = s1recv[:, span].astype(F32)
        before = s2recv[:, span].astype(F32)

        @pl.when(a < groups - 1)
        def _(p=p, span=span, total=before + own + paired):
            s2send[:, span] = total.astype(BF16)
            chain[p].start()

        s3send[:, span] = (before + jnp.where(b == 0, own, 0.0)).astype(BF16)
        back[p].start()
        memory[mine, span] = (before + jnp.where(b == 1, paired, 0.0)).astype(BF16)

    for h in range(heads):
        attention(CHUNKS - 1, h)

    to_mix = [
        remote(
            mix.at[rows(i), pl.ds(0, width)], mix.at[rows(i), pl.ds(width, width)], mix_s.at[i], mix_r.at[i], head=sib
        )
        for i in range(CHUNKS)
    ]
    to_p = [remote(psend.at[rows(i), :], precv.at[rows(i), :], p_s.at[i], p_r.at[i], head=cross) for i in range(CHUNKS)]
    to_out = [pltpu.make_async_copy(outv.at[rows(i), :], out.at[rows(i), :], out_sem.at[i]) for i in range(CHUNKS)]

    def readout(i):
        for h in range(heads):
            cols = pl.ds(h * hsize, hsize)
            share = jax.nn.sigmoid(jnp.full((1, hsize), logit[h], F32))
            fquery = feature(q[rows(i), cols].astype(F32)).astype(BF16)
            numer = matmul(fquery, memory[h, pl.ds(0, hsize), :])
            normal = memory[h, pl.ds(hsize, PAD), :].astype(F32)[0:1]
            denom = jnp.sum(fquery.astype(F32) * normal, axis=1, keepdims=True)
            read = numer / jnp.maximum(denom, 1.0)
            mix[rows(i), cols] = (share * read + (1.0 - share) * loc[rows(i), cols]).astype(BF16)
        to_mix[i].start()

    def partial(i):
        to_mix[i].wait_recv()
        if i == 0:
            for copy in own_wo:
                copy.wait()
            for copy in to_wos:
                copy.wait_recv()
        psend[rows(i), :] = matmul(mix[rows(i), :], wos[:, pl.ds(feats, feats)]).astype(BF16)
        to_p[i].start()

    for copy in back:
        copy.wait_recv()
    readout(0)
    for i in range(1, CHUNKS):
        readout(i)
        partial(i - 1)
    partial(CHUNKS - 1)
    for i in range(CHUNKS):
        own = matmul(mix[rows(i), :], wos[:, pl.ds(0, feats)])
        to_p[i].wait_recv()
        outv[rows(i), :] = (own + precv[rows(i), :].astype(F32)).astype(BF16)
        to_out[i].start()

    for i in range(CHUNKS):
        for copies in (to_cross, to_sib, forward, to_mix, to_p):
            copies[i].wait_send()
    for copy in to_wos + swap + back:
        copy.wait_send()
    @pl.when(a < groups - 1)
    def _():
        for copy in chain:
            copy.wait_send()

    for copy in to_out:
        copy.wait()


def on_device(groups, tokens, w_query, w_key, w_value, w_out, mix_logit):
    seg, feats = tokens.shape
    depth, width = w_query.shape
    heads = mix_logit.shape[0]
    hsize = width // heads
    half = heads // 2
    dma = pltpu.SemaphoreType.DMA
    piece = (half, hsize + PAD, hsize)
    anywhere = pl.BlockSpec(memory_space=pl.ANY)
    return pl.pallas_call(
        functools.partial(kernel, groups),
        out_shape=jax.ShapeDtypeStruct((seg, feats), BF16),
        in_specs=[anywhere] * 5 + [pl.BlockSpec(memory_space=pltpu.SMEM)],
        out_specs=anywhere,
        scratch_shapes=[
            pltpu.VMEM((seg, depth), BF16),
            pltpu.VMEM((3, depth, width), BF16),
            pltpu.VMEM((2 * width, 2 * feats), BF16),
            pltpu.VMEM((seg, width), BF16),
            pltpu.VMEM((seg, width), BF16),
            pltpu.VMEM((seg, width), BF16),
            pltpu.VMEM((seg, width), F32),
            pltpu.VMEM((seg, 2 * width), BF16),
            pltpu.VMEM((seg, feats), BF16),
            pltpu.VMEM((seg, feats), BF16),
            pltpu.VMEM((seg, feats), BF16),
            pltpu.VMEM((heads, hsize + PAD, hsize), F32),
            pltpu.VMEM(piece, BF16),
            pltpu.VMEM(piece, BF16),
            pltpu.VMEM(piece, BF16),
            pltpu.VMEM(piece, BF16),
            pltpu.VMEM(piece, BF16),
            pltpu.VMEM((heads, hsize + PAD, hsize), BF16),
            dma((CHUNKS,)),
            dma((3, 4)),
            dma((2,)),
            dma((2,)),
            dma((2,)),
        ]
        + [dma((CHUNKS,))] * 6
        + [dma((PIECES,))] * 6
        + [dma((CHUNKS,))] * 5,
        compiler_params=pltpu.CompilerParams(collective_id=0, has_side_effects=True, vmem_limit_bytes=64000000),
    )(tokens, w_query, w_key, w_value, w_out, mix_logit)


def solution(mesh):
    placed = (
        P("seq", "head"),
        P(None, "head"),
        P(None, "head"),
        P(None, "head"),
        P("head", None),
        P("head"),
    )
    return jax.shard_map(
        functools.partial(on_device, mesh.shape["seq"] // 2),
        mesh=mesh,
        in_specs=placed,
        out_specs=P("seq", "head"),
        check_vma=False,
    )
```
